128 devices in a mesh: samp: 8 (over x, core), feat: 16 (over z, y).
Axes of the slice: x: 4, y: 4, z: 4, core: 2. Of those that a mesh axis runs over, the one named last changes fastest.
Arguments:
- design: float32 [8192, 65536], P('samp', 'feat'), may hold values from -0.06629126 to 0.06629126
- coefficients: float32 [192, 65536], P(None, 'feat'), may hold values from -4 to 4
- response: float32 [192, 8192], P(None, 'samp'), may hold values from -6 to 6
- active_set: int32 [192, 65536], P(None, 'feat'), may hold values 0 or 1
- lambda_path: float32 [192, 16], P('samp'), may hold values from 0.5 to 4
- lambda_index: int32 [192], P('samp'), may hold values from 1 to 15
Outputs:
- margins: float32 [192, 65536], P('samp', 'feat')
- peak_gradient: float32 [192], P('samp')
- violation: float32 [192], P('samp')
- screen_mass: float32 [192], P('samp')
The draws below stay inside these ranges and needn't reach their ends.
Inputs may be any that keep to these rules, and one draw needn't show every extreme that they name: `active_set`: 1 marks a feature in the response's active set, 0 one outside it. `lambda_index`: the current point on the response's path; the previous point is the one just below it.
All inputs are finite; a program needn't handle non-finite values. No bound on the sum of `active_set` on one device may be relied on, other than what follows from the above.
Results may differ from the reference program's by a relative error of at most 0.000073.
Values sent between devices are 32-bit elements; how exact they have to be, the bound alone decides.
A program may use at most 128 MiB of HBM per device.

```python
import math
import jax
import jax.numpy as jnp
from jax import lax

NF = 65536
R = 192
L = 16
NS = 8192


def plant(result, stream_key, smallest, largest):
    longest = result.shape.index(max(result.shape))
    spots = []
    for shift in (0, 1):
        where = [jax.random.randint(jax.random.fold_in(stream_key, axis), (), 0, length) for axis, length in enumerate(result.shape)]
        where[longest] = (where[longest] + shift) % result.shape[longest]
        spots.append(tuple(where))
    return result.at[spots[0]].set(smallest).at[spots[1]].set(largest)


def level_of(stream_key, dims, pieces, low, largest):
    gain = 1.0
    for position, parts in pieces:
        draws = jax.random.uniform(jax.random.fold_in(jax.random.fold_in(stream_key, 6), position), (parts,), jnp.float32, low / len(pieces), largest / len(pieces))
        gain = gain * jnp.repeat(jnp.exp(draws), dims[position] // parts).reshape((-1,) + (1,) * (len(dims) - 1 - position))
    return gain


def noise(stream_key, dims, deviation, reach, pieces=(), kind=jnp.bfloat16):
    factor_of = level_of(stream_key, dims, pieces, -0.22, 0.18) if pieces else 1.0
    entries = jax.random.normal(stream_key, dims, jnp.float32) * deviation * factor_of
    return jnp.minimum(jnp.maximum(entries, -reach), reach).astype(kind)


def setup_inputs(seed: int = 0) -> dict:
    key_list = jax.random.split(jax.random.key(seed), 7)
    design = noise(key_list[0], (NS, NF), (NS ** -0.5), 0.06629126, ((0, 8), (1, 16)), jnp.float32)
    coefficients = noise(key_list[1], (R, NF), (2.0 * NS ** 0.5 / NF ** 0.5), 4.0, ((1, 16),), jnp.float32)
    response = noise(key_list[2], (R, NS), 1.0, 6.0, ((1, 8),), jnp.float32)
    active_set = plant((jax.random.randint(key_list[3], (R, NF), 0, 4) < 1).astype(jnp.int32), jax.random.fold_in(key_list[3], 1), 0, 1)
    lambda_path = jnp.clip(jnp.exp(math.log(4.0) - 2.0794415 * jax.random.uniform(key_list[4], (R, L), jnp.float32) ** level_of(key_list[4], (R, L), ((0, 8),), -0.2, 0.2)), 0.5, 4.0)
    lambda_index = plant(jax.random.randint(key_list[5], (R,), 1, L), jax.random.fold_in(key_list[5], 1), 1, L - 1).astype(jnp.int32)
    return dict(design=design, coefficients=coefficients, response=response, active_set=active_set, lambda_path=lambda_path, lambda_index=lambda_index)


def reference(design, coefficients, response, active_set, lambda_path, lambda_index):
    masked = coefficients * active_set.astype(jnp.float32)
    fitted = lax.dot_general(masked, design, (((1,), (1,)), ((), ())), precision=lax.Precision.HIGHEST, preferred_element_type=jnp.float32)
    residual = response - fitted
    gradient = jnp.dot(residual, design, precision=lax.Precision.HIGHEST, preferred_element_type=jnp.float32)
    positions = jnp.arange(lambda_path.shape[1], dtype=jnp.int32)
    picker_now = (positions[None, :] == lambda_index[:, None]).astype(jnp.float32)
    picker_before = (positions[None, :] == (lambda_index[:, None] - 1)).astype(jnp.float32)
    lambda_new = jnp.sum(lambda_path * picker_now, axis=1)
    lambda_old = jnp.sum(lambda_path * picker_before, axis=1)
    threshold = 2.0 * lambda_new - lambda_old
    magnitude = jnp.abs(gradient)
    margins = magnitude - threshold[:, None]
    peak_gradient = jnp.max(magnitude, axis=1)
    inactive = 1.0 - active_set.astype(jnp.float32)
    violation = jnp.sum(inactive * jnp.maximum(magnitude - lambda_new[:, None], 0.0), axis=1) / NF
    screen_mass = jnp.sum(jnp.maximum(margins, 0.0), axis=1) / NF
    return (margins, peak_gradient, violation, screen_mass)
```

```python
import functools

import jax
import jax.numpy as jnp
from jax import lax
from jax.experimental import pallas as pl
from jax.experimental.pallas import tpu as pltpu
from jax.sharding import PartitionSpec as P

NF = 65536
F32 = jnp.float32
BF16 = jnp.bfloat16
CHUNKS = 4
PARTS = 8


def split(value):
    high = value.astype(BF16)
    return high, (value - high.astype(F32)).astype(BF16)


def dot(a, b):
    return jnp.dot(a, b, preferred_element_type=F32)


def kernel(
    design, coefficients, response, active, lpath, lindex,
    margins, stats,
    raw, d_hi, d_lo, coef, act, resp, m_hi, m_lo,
    part, got1, summed, got2, resid, a_hi, a_lo,
    grad, got_core, got_hop, got_end, peers,
    load_sem, s1, r1, s2, r2, s3, r3, sc, rc, sx, rx, st, rt,
):
    samp = lax.axis_index("samp")
    feat = lax.axis_index("feat")
    x, core = samp // 2, samp % 2
    z, y = feat // 4, feat % 4
    rows, samples = response.shape
    features = design.shape[1]
    share = rows // 8
    height = samples // CHUNKS
    slab = rows // 4
    width = features // PARTS
    half = width // 2

    def to(s, f):
        return dict(device_id=(s, f), device_id_type=pl.DeviceIdType.MESH)

    partner = 2 * x + 1 - core
    left = 2 * ((x + 3) % 4) + core
    right = 2 * ((x + 1) % 4) + core

    loads = [
        pltpu.make_async_copy(coefficients, coef, load_sem.at[0]),
        pltpu.make_async_copy(active, act, load_sem.at[1]),
    ]
    for c in range(CHUNKS):
        area = pl.ds(c * height, height)
        loads.append(pltpu.make_async_copy(design.at[area], raw.at[area], load_sem.at[3 + c]))
    loads.append(pltpu.make_async_copy(response, resp, load_sem.at[2]))
    for load in loads:
        load.start()

    barrier = pltpu.get_barrier_semaphore()
    for k in range(1, 16):
        pl.semaphore_signal(barrier, inc=1, **to(samp, (feat + k) % 16))
    for s in (partner, left, right):
        pl.semaphore_signal(barrier, inc=1, **to(s, feat))

    loads[0].wait()
    loads[1].wait()

    def mask_step(b, carry):
        area = pl.ds(pl.multiple_of(b * 512, 512), 512)
        hi, lo = split((coef[:, area] * act[:, area].astype(F32)).T)
        m_hi[area, :] = hi
        m_lo[area, :] = lo
        return carry

    lax.fori_loop(0, features // 512, mask_step, 0)

    def along(color, k):
        return 4 * z + (y + k) % 4 if color == 0 else 4 * ((z + k) % 4) + y

    def place(color):
        return y if color == 0 else z

    def slab_of(a):
        return pl.ds(pl.multiple_of(a * slab, slab), slab)

    def send1(c, color, k):
        a = (place(color) + k) % 4
        return pltpu.make_async_remote_copy(
            part.at[c, color, slab_of(a)], got1.at[c, color, k - 1],
            s1.at[c, color, k - 1], r1.at[c, color, k - 1], **to(samp, along(color, k)))

    def send2(c, color, k):
        return pltpu.make_async_remote_copy(
            summed.at[c, color], got2.at[c, color, k - 1],
            s2.at[c, color, k - 1], r2.at[c, color, k - 1], **to(samp, along(1 - color, k)))

    def lanes_of(c, color):
        return pl.ds(c * height + color * 128, 128)

    def send3(c, color, k):
        area = resid.at[slab_of(place(color)), lanes_of(c, color)]
        return pltpu.make_async_remote_copy(
            area, area,
            s3.at[c, color, k - 1], r3.at[c, color, k - 1], **to(samp, along(color, k)))

    for c in range(CHUNKS):
        loads[2 + c].wait()
        area = pl.ds(c * height, height)
        hi, lo = split(raw[area, :])
        d_hi[area, :] = hi
        d_lo[area, :] = lo
        fitted = dot(d_hi[area, :], m_hi[...]) + dot(d_hi[area, :], m_lo[...]) + dot(d_lo[area, :], m_hi[...])
        fitted = fitted.T
        part[c, 0] = fitted[:, :128]
        part[c, 1] = fitted[:, 128:]
        if c == 0:
            pl.semaphore_wait(barrier, 18)
        for k in (2, 1, 3):
            for color in (0, 1):
                send1(c, color, k).start()

    loads[2 + CHUNKS].wait()
    for c in range(CHUNKS):
        for color in (0, 1):
            for k in (1, 2, 3):
                send1(c, color, k).wait_recv()
            summed[c, color] = (part[c, color, slab_of(place(color)), :] + got1[c, color, 0]) + (
                got1[c, color, 1] + got1[c, color, 2])
            for k in (2, 1, 3):
                send2(c, color, k).start()
    for c in range(CHUNKS):
        for color in (0, 1):
            for k in (1, 2, 3):
                send2(c, color, k).wait_recv()
            total = (summed[c, color] + got2[c, color, 0]) + (got2[c, color, 1] + got2[c, color, 2])
            mine, lanes = slab_of(place(color)), lanes_of(c, color)
            resid[mine, lanes] = resp[mine, lanes] - total
            for k in (2, 1, 3):
                send3(c, color, k).start()
    for c in range(CHUNKS):
        for color in (0, 1):
            for k in (1, 2, 3):
                send3(c, color, k).wait_recv()
        area = pl.ds(c * height, height)
        hi, lo = split(resid[:, area])
        a_hi[:, area] = hi
        a_lo[:, area] = lo

    eye = lax.broadcasted_iota(jnp.int32, (share, share), 0) == lax.broadcasted_iota(jnp.int32, (share, share), 1)
    index = jnp.sum(jnp.where(eye, jnp.broadcast_to(lindex[...], (share, share)).astype(F32), 0.0), axis=1, keepdims=True)
    positions = lax.broadcasted_iota(jnp.int32, lpath.shape, 1).astype(F32)
    path = lpath[...]
    lam_new = jnp.sum(jnp.where(positions == index, path, 0.0), axis=1, keepdims=True)
    lam_old = jnp.sum(jnp.where(positions == index - 1.0, path, 0.0), axis=1, keepdims=True)
    threshold = 2.0 * lam_new - lam_old

    def send_core(q):
        return pltpu.make_async_remote_copy(
            grad.at[q, :, 1 - core], got_core.at[q], sc.at[q], rc.at[q], **to(partner, feat))

    near = pl.ds(0, half)
    far = pl.ds(half, half)
    x_left, x_right, x_far = (x + 3) % 4, (x + 1) % 4, (x + 2) % 4

    def send_x(q, kind):
        source, target, where = (
            (grad.at[q, x_far, core, :, near], got_hop.at[q, 0], left),
            (grad.at[q, x_far, core, :, far], got_hop.at[q, 1], right),
            (grad.at[q, x_left, core, :, far], got_end.at[q, 0, :, far], left),
            (grad.at[q, x_right, core, :, near], got_end.at[q, 1, :, near], right),
            (grad.at[q, x_left, core, :, near], got_end.at[q, 0, :, near], left),
            (grad.at[q, x_right, core, :, far], got_end.at[q, 1, :, far], right),
        )[kind]
        return pltpu.make_async_remote_copy(source, target, sx.at[q, kind], rx.at[q, kind], **to(where, feat))

    def multiply(q):
        cols = pl.ds(q * width, width)
        right_hi = d_hi[:, cols]
        value = dot(a_hi[...], right_hi) + dot(a_lo[...], right_hi) + dot(a_hi[...], d_lo[:, cols])
        for j in range(8):
            grad[q, j // 2, j % 2] = value[j * share:(j + 1) * share, :]
        send_core(q).start()

    def first_hop(q):
        send_core(q).wait_recv()
        for j in range(4):
            grad[q, j, core] = grad[q, j, core] + got_core[q, j]
        for kind in (0, 1, 2, 3):
            send_x(q, kind).start()

    def second_hop(q):
        send_x(q, 0).wait_recv()
        send_x(q, 1).wait_recv()
        grad[q, x_left, core, :, near] = grad[q, x_left, core, :, near] + got_hop[q, 0]
        grad[q, x_right, core, :, far] = grad[q, x_right, core, :, far] + got_hop[q, 1]
        send_x(q, 4).start()
        send_x(q, 5).start()

    own_rows = pl.ds(pl.multiple_of(samp * share, share), share)

    def finish(q, carry):
        peak, violation, mass = carry
        for kind in (2, 3, 4, 5):
            send_x(q, kind).wait_recv()
        cols = pl.ds(q * width, width)
        magnitude = jnp.abs(grad[q, x, core] + (got_end[q, 0] + got_end[q, 1]))
        margin = magnitude - threshold
        margins[:, cols] = margin
        excess = (1.0 - act[own_rows, cols].astype(F32)) * jnp.maximum(magnitude - lam_new, 0.0)
        positive = jnp.maximum(margin, 0.0)
        for j in range(0, width, 128):
            peak = jnp.maximum(peak, magnitude[:, j:j + 128])
            violation = violation + excess[:, j:j + 128]
            mass = mass + positive[:, j:j + 128]
        return peak, violation, mass

    carry = tuple(jnp.zeros((share, 128), F32) for _ in range(3))
    for q in range(PARTS):
        multiply(q)
        if q >= 1:
            first_hop(q - 1)
    first_hop(PARTS - 1)
    for q in range(PARTS):
        second_hop(q)
    for q in range(PARTS):
        carry = finish(q, carry)

    peak, violation, mass = carry
    lane = lax.broadcasted_iota(jnp.int32, (share, 128), 1)
    packed = jnp.where(
        lane == 0, jnp.max(peak, axis=1, keepdims=True),
        jnp.where(
            lane == 1, jnp.sum(violation, axis=1, keepdims=True) * (1.0 / NF),
            jnp.where(lane == 2, jnp.sum(mass, axis=1, keepdims=True) * (1.0 / NF), 0.0)))
    packed = jnp.concatenate([packed, jnp.zeros((128 - share, 128), F32)], axis=0).T
    peers[feat] = packed[:8, :]

    def send_stats(k):
        return pltpu.make_async_remote_copy(
            peers.at[feat], peers.at[feat], st.at[k], rt.at[k], **to(samp, (feat + k) % 16))

    for k in range(1, 16):
        send_stats(k).start()
    for k in range(1, 16):
        send_stats(k).wait_recv()
    everything = [peers[k] for k in range(16)]
    largest, total = everything[0], everything[0]
    for k in range(1, 16):
        largest = jnp.maximum(largest, everything[k])
        total = total + everything[k]
    stats[...] = jnp.where(lax.broadcasted_iota(jnp.int32, (8, 128), 0) == 0, largest, total)

    for c in range(CHUNKS):
        for color in (0, 1):
            for k in (1, 2, 3):
                send1(c, color, k).wait_send()
                send2(c, color, k).wait_send()
                send3(c, color, k).wait_send()
    for q in range(PARTS):
        send_core(q).wait_send()
        for kind in range(6):
            send_x(q, kind).wait_send()
    for k in range(1, 16):
        send_stats(k).wait_send()


def body(design, coefficients, response, active_set, lambda_path, lambda_index):
    samples, features = design.shape
    rows = coefficients.shape[0]
    share = lambda_path.shape[0]
    height, slab, width = samples // CHUNKS, rows // 4, features // PARTS
    vmem = pltpu.VMEM
    dma = pltpu.SemaphoreType.DMA
    everywhere = pl.BlockSpec(memory_space=pl.ANY)
    inside = pl.BlockSpec(memory_space=pltpu.VMEM)
    margins, stats = pl.pallas_call(
        kernel,
        out_shape=(
            jax.ShapeDtypeStruct((share, features), F32),
            jax.ShapeDtypeStruct((8, 128), F32),
        ),
        in_specs=[everywhere] * 4 + [inside] * 2,
        out_specs=(inside, inside),
        scratch_shapes=[
            vmem((samples, features), F32),
            vmem((samples, features), BF16),
            vmem((samples, features), BF16),
            vmem((rows, features), F32),
            vmem((rows, features), jnp.int32),
            vmem((rows, samples), F32),
            vmem((features, rows), BF16),
            vmem((features, rows), BF16),
            vmem((CHUNKS, 2, rows, 128), F32),
            vmem((CHUNKS, 2, 3, slab, 128), F32),
            vmem((CHUNKS, 2, slab, 128), F32),
            vmem((CHUNKS, 2, 3, slab, 128), F32),
            vmem((rows, samples), F32),
            vmem((rows, samples), BF16),
            vmem((rows, samples), BF16),
            vmem((PARTS, 4, 2, share, width), F32),
            vmem((PARTS, 4, share, width), F32),
            vmem((PARTS, 2, share, width // 2), F32),
            vmem((PARTS, 2, share, width), F32),
            vmem((16, 8, 128), F32),
            dma((3 + CHUNKS,)),
            *[dma((CHUNKS, 2, 3))] * 6,
            *[dma((PARTS,))] * 2,
            *[dma((PARTS, 6))] * 2,
            *[dma((16,))] * 2,
        ],
        compiler_params=pltpu.CompilerParams(
            collective_id=0, has_side_effects=True, vmem_limit_bytes=67043328
        ),
    )(design, coefficients, response, active_set, lambda_path, lambda_index.reshape(1, share))
    return margins, stats[0, :share], stats[1, :share], stats[2, :share]


def solution(mesh):
    return jax.shard_map(
        body,
        mesh=mesh,
        in_specs=(
            P("samp", "feat"),
            P(None, "feat"),
            P(None, "samp"),
            P(None, "feat"),
            P("samp", None),
            P("samp"),
        ),
        out_specs=(P("samp", "feat"), P("samp"), P("samp"), P("samp")),
        check_vma=False,
    )
```

```python
import functools

import jax
import jax.numpy as jnp
from jax import lax
from jax.experimental import pallas as pl
from jax.experimental.pallas import tpu as pltpu
from jax.sharding import PartitionSpec as P

NF = 65536
F32 = jnp.float32
BF16 = jnp.bfloat16
CHUNKS = 8
LAG = 4
BLOCKS = 4
WIDTHS = (512,) * 8
PARTS = len(WIDTHS)
STARTS = tuple(sum(WIDTHS[:k]) for k in range(PARTS))


def split(value):
    high = value.astype(BF16)
    return high, (value - high.astype(F32)).astype(BF16)


def dot(a, b):
    return jnp.dot(a, b, preferred_element_type=F32)


def kernel(
    design, coefficients, response, active, lpath, lindex,
    margins, stats,
    raw, d_all, coef, act, resp, m_hi, m_lo,
    part, got1, summed, got2, resid, a_all,
    grad, got_core, got_hop, got_end, lams, peers,
    coef_sem, act_sem, load_sem, sent, r1, r2, r3, rc, rx, rt,
):
    samp = lax.axis_index("samp")
    feat = lax.axis_index("feat")
    x, core = samp // 2, samp % 2
    z, y = feat // 4, feat % 4
    rows, samples = response.shape
    features = design.shape[1]
    share = rows // 8
    height = samples // CHUNKS
    slab = rows // 8

    def to(s, f):
        return dict(device_id=(s, f), device_id_type=pl.DeviceIdType.MESH)

    partner = 2 * x + 1 - core
    left = 2 * ((x + 3) % 4) + core
    right = 2 * ((x + 1) % 4) + core

    step = features // BLOCKS

    def load_block(b):
        area = pl.ds(pl.multiple_of(b * step, step), step)
        return (
            pltpu.make_async_copy(coefficients.at[:, area], coef.at[:, area], coef_sem.at[b]),
            pltpu.make_async_copy(active.at[:, area], act.at[:, area], act_sem.at[b]))

    def load_design(c):
        area = pl.ds(pl.multiple_of(c * height, height), height)
        return pltpu.make_async_copy(design.at[area], raw.at[area], load_sem.at[c])

    load_response = pltpu.make_async_copy(response, resp, load_sem.at[CHUNKS])
    for b in range(BLOCKS):
        for load in load_block(b):
            load.start()

    barrier = pltpu.get_barrier_semaphore()
    for k in range(1, 16):
        pl.semaphore_signal(barrier, inc=1, **to(samp, (feat + k) % 16))
    for s in (partner, left, right):
        pl.semaphore_signal(barrier, inc=1, **to(s, feat))

    eye = lax.broadcasted_iota(jnp.int32, (share, share), 0) == lax.broadcasted_iota(jnp.int32, (share, share), 1)
    positions = lax.broadcasted_iota(jnp.int32, lpath.shape, 0)
    index, path = lindex[...], lpath[...]

    def pick(chosen):
        row = jnp.sum(jnp.where(positions == chosen, path, 0.0), axis=0, keepdims=True)
        return jnp.sum(jnp.where(eye, jnp.broadcast_to(row, (share, share)), 0.0), axis=1, keepdims=True)

    lam_new, lam_old = pick(index), pick(index - 1)
    lams[0] = jnp.broadcast_to(lam_new, (share, 128))
    lams[1] = jnp.broadcast_to(2.0 * lam_new - lam_old, (share, 128))

    @jax.named_scope("mask")
    def mask_step(b, carry):
        for load in load_block(b):
            load.wait()
        area = pl.ds(pl.multiple_of(b * step, step), step)
        hi, lo = split((coef[:, area] * act[:, area].astype(F32)).T)
        m_hi[area, :] = hi
        m_lo[area, :] = lo
        return carry

    lax.fori_loop(0, 1, mask_step, 0)
    load_design(0).start()
    lax.fori_loop(1, 2, mask_step, 0)
    load_design(1).start()
    lax.fori_loop(2, BLOCKS, mask_step, 0)
    for c in range(2, CHUNKS):
        load_design(c).start()
    load_response.start()

    def along(color, k):
        return 4 * z + (y + k) % 4 if color == 0 else 4 * ((z + k) % 4) + y

    def place(color):
        return y if color == 0 else z

    def slab_of(color, a):
        return pl.ds(pl.multiple_of((color * 4 + a) * slab, slab), slab)

    def lanes_of(c):
        return pl.ds(pl.multiple_of(c * height, height), height)

    def send1(c, color, k):
        a = (place(color) + k) % 4
        return pltpu.make_async_remote_copy(
            part.at[c, slab_of(color, a)], got1.at[c, color, k - 1],
            sent.at[0], r1.at[c], **to(samp, along(color, k)))

    def send2(c, color, k):
        return pltpu.make_async_remote_copy(
            summed.at[c, color], got2.at[c, color, k - 1],
            sent.at[1], r2.at[c], **to(samp, along(1 - color, k)))

    def send3(c, color, k):
        area = resid.at[slab_of(color, place(color)), lanes_of(c)]
        return pltpu.make_async_remote_copy(
            area, area,
            sent.at[2], r3.at[c], **to(samp, along(color, k)))

    def await_bytes(ref, sem):
        pltpu.make_async_copy(ref, ref, sem).wait()

    def phase1(c):
        await_bytes(got1.at[c], r1.at[c])
        for color in (0, 1):
            summed[c, color] = (part[c, slab_of(color, place(color)), :] + got1[c, color, 0]) + (
                got1[c, color, 1] + got1[c, color, 2])
            for k in (2, 1, 3):
                send2(c, color, k).start()

    def phase2(c):
        await_bytes(got2.at[c], r2.at[c])
        for color in (0, 1):
            total = (summed[c, color] + got2[c, color, 0]) + (got2[c, color, 1] + got2[c, color, 2])
            mine, lanes = slab_of(color, place(color)), lanes_of(c)
            resid[mine, lanes] = resp[mine, lanes] - total
            for k in (2, 1, 3):
                send3(c, color, k).start()

    def phase3(c):
        await_bytes(got2.at[c], r3.at[c])
        hi, lo = split(resid[:, lanes_of(c)])
        a_all[:rows, lanes_of(c)] = hi
        a_all[rows:, lanes_of(c)] = lo

    @jax.named_scope("fit")
    def fit_step(c, carry):
        load_design(c).wait()
        area = pl.ds(pl.multiple_of(c * height, height), height)
        hi, lo = split(raw[area, :])
        d_all[c, 0] = hi
        d_all[c, 1] = lo
        both = dot(d_all[c].reshape(2 * height, features), m_hi[...])
        part[c] = (both[:height] + both[height:] + dot(d_all[c, 0], m_lo[...])).T

        @pl.when(c == 0)
        def _():
            pl.semaphore_wait(barrier, 18)

        for k in (2, 1, 3):
            for color in (0, 1):
                send1(c, color, k).start()

        @pl.when(c >= LAG)
        def _():
            phase1(c - LAG)

        return carry

    lax.fori_loop(0, CHUNKS, fit_step, 0)
    with jax.named_scope("phase12"):
        load_response.wait()
        for c in range(CHUNKS):
            if c + CHUNKS - LAG < CHUNKS:
                phase1(c + CHUNKS - LAG)
            phase2(c)
    x_left, x_right, x_far = (x + 3) % 4, (x + 1) % 4, (x + 2) % 4

    def cols_of(q):
        return pl.ds(STARTS[q], WIDTHS[q])

    def halves_of(q):
        half = WIDTHS[q] // 2
        return pl.ds(STARTS[q], half), pl.ds(STARTS[q] + half, half), pl.ds(STARTS[q] // 2, half)

    def send_core(q):
        return pltpu.make_async_remote_copy(
            grad.at[:, 1 - core, :, cols_of(q)], got_core.at[:, :, cols_of(q)], sent.at[3], rc.at[q], **to(partner, feat))

    def send_x(q, kind):
        near, far, packed = halves_of(q)
        source, target, where = (
            (grad.at[x_far, core, :, near], got_hop.at[0, :, packed], left),
            (grad.at[x_far, core, :, far], got_hop.at[1, :, packed], right),
            (grad.at[x_left, core, :, far], got_end.at[0, :, far], left),
            (grad.at[x_right, core, :, near], got_end.at[1, :, near], right),
            (grad.at[x_left, core, :, near], got_end.at[0, :, near], left),
            (grad.at[x_right, core, :, far], got_end.at[1, :, far], right),
        )[kind]
        return pltpu.make_async_remote_copy(source, target, sent.at[4], rx.at[q, min(kind, 2)], **to(where, feat))

    @jax.named_scope("multiply")
    def multiply(q, first, last):
        cols = cols_of(q)
        depth, width = (last - first) * height, WIDTHS[q]
        left_all = a_all[:, first * height:last * height]
        both = dot(left_all, d_all[first:last, 0, :, cols].reshape(depth, width))
        value = both[:rows] + both[rows:] + dot(left_all[:rows], d_all[first:last, 1, :, cols].reshape(depth, width))
        for j in range(8):
            piece = value[j * share:(j + 1) * share, :]
            if first > 0:
                piece = piece + grad[j // 2, j % 2, :, cols]
            grad[j // 2, j % 2, :, cols] = piece
        if last == CHUNKS:
            send_core(q).start()

    @jax.named_scope("hop1")
    def first_hop(q):
        cols = cols_of(q)
        send_core(q).wait_recv()
        for j in (x_far, x_left, x_right, x):
            grad[j, core, :, cols] = grad[j, core, :, cols] + got_core[j, :, cols]
        for kind in (0, 1, 2, 3):
            send_x(q, kind).start()

    @jax.named_scope("hop2")
    def second_hop(q):
        near, far, packed = halves_of(q)
        send_x(q, 0).wait_recv()
        grad[x_left, core, :, near] = grad[x_left, core, :, near] + got_hop[0, :, packed]
        send_x(q, 4).start()
        send_x(q, 1).wait_recv()
        grad[x_right, core, :, far] = grad[x_right, core, :, far] + got_hop[1, :, packed]
        send_x(q, 5).start()

    own_rows = pl.ds(pl.multiple_of(samp * share, share), share)

    @jax.named_scope("finish")
    def finish(q, carry):
        peak, violation, mass = carry
        await_bytes(got_end.at[:, :, cols_of(q)], rx.at[q, 2])
        for j in range(STARTS[q], STARTS[q] + WIDTHS[q], 128):
            cols = pl.ds(j, 128)
            magnitude = jnp.abs(grad[x, core, :, cols] + (got_end[0, :, cols] + got_end[1, :, cols]))
            margin = magnitude - lams[1]
            margins[:, cols] = margin
            peak = jnp.maximum(peak, magnitude)
            violation = violation + (1.0 - act[own_rows, cols].astype(F32)) * jnp.maximum(magnitude - lams[0], 0.0)
            mass = mass + jnp.maximum(margin, 0.0)
        return peak, violation, mass

    carry = tuple(jnp.zeros((share, 128), F32) for _ in range(3))
    with jax.named_scope("phase3"):
        for c in range(CHUNKS):
            phase3(c)
            if c == CHUNKS // 2:
                multiply(0, 0, CHUNKS // 2)
    multiply(0, CHUNKS // 2, CHUNKS)
    for q in range(PARTS):
        if q >= 1:
            multiply(q, 0, CHUNKS)
            first_hop(q - 1)
    first_hop(PARTS - 1)
    for q in range(PARTS):
        second_hop(q)
    for q in range(PARTS):
        carry = finish(q, carry)

    with jax.named_scope("stats"):
        peak, violation, mass = carry
        lane = lax.broadcasted_iota(jnp.int32, (share, 128), 1)
        packed = jnp.where(
            lane == 0, jnp.max(peak, axis=1, keepdims=True),
            jnp.where(
                lane == 1, jnp.sum(violation, axis=1, keepdims=True) * (1.0 / NF),
                jnp.where(lane == 2, jnp.sum(mass, axis=1, keepdims=True) * (1.0 / NF), 0.0)))
        packed = jnp.concatenate([packed, jnp.zeros((128 - share, 128), F32)], axis=0).T
        peers[feat] = packed[:8, :]

        def send_stats(k):
            return pltpu.make_async_remote_copy(
                peers.at[feat], peers.at[feat], sent.at[5], rt.at[0], **to(samp, (feat + k) % 16))

        for k in range(1, 16):
            send_stats(k).start()
        await_bytes(peers.at[pl.ds(0, 15)], rt.at[0])
        everything = [peers[k] for k in range(16)]
        largest, total = everything[0], everything[0]
        for k in range(1, 16):
            largest = jnp.maximum(largest, everything[k])
            total = total + everything[k]
        stats[...] = jnp.where(lax.broadcasted_iota(jnp.int32, (8, 128), 0) == 0, largest, total)

    await_bytes(got1, sent.at[0])
    await_bytes(got1, sent.at[1])
    await_bytes(got1, sent.at[2])
    await_bytes(got_core, sent.at[3])
    await_bytes(got_hop, sent.at[4])
    await_bytes(got_end, sent.at[4])
    await_bytes(peers.at[pl.ds(0, 15)], sent.at[5])


def body(design, coefficients, response, active_set, lambda_path, lambda_index):
    samples, features = design.shape
    rows = coefficients.shape[0]
    share = lambda_path.shape[0]
    height, slab = samples // CHUNKS, rows // 8
    vmem = pltpu.VMEM
    dma = pltpu.SemaphoreType.DMA
    everywhere = pl.BlockSpec(memory_space=pl.ANY)
    inside = pl.BlockSpec(memory_space=pltpu.VMEM)
    margins, stats = pl.pallas_call(
        kernel,
        out_shape=(
            jax.ShapeDtypeStruct((share, features), F32),
            jax.ShapeDtypeStruct((8, 128), F32),
        ),
        in_specs=[everywhere] * 4 + [inside] * 2,
        out_specs=(inside, inside),
        scratch_shapes=[
            vmem((samples, features), F32),
            vmem((CHUNKS, 2, height, features), BF16),
            vmem((rows, features), F32),
            vmem((rows, features), jnp.int32),
            vmem((rows, samples), F32),
            vmem((features, rows), BF16),
            vmem((features, rows), BF16),
            vmem((CHUNKS, rows, height), F32),
            vmem((CHUNKS, 2, 3, slab, height), F32),
            vmem((CHUNKS, 2, slab, height), F32),
            vmem((CHUNKS, 2, 3, slab, height), F32),
            vmem((rows, samples), F32),
            vmem((2 * rows, samples), BF16),
            vmem((4, 2, share, features), F32),
            vmem((4, share, features), F32),
            vmem((2, share, features // 2), F32),
            vmem((2, share, features), F32),
            vmem((2, share, 128), F32),
            vmem((16, 8, 128), F32),
            dma((BLOCKS,)),
            dma((BLOCKS,)),
            dma((CHUNKS + 1,)),
            dma((6,)),
            *[dma((CHUNKS,))] * 3,
            dma((PARTS,)),
            dma((PARTS, 3)),
            dma((1,)),
        ],
        compiler_params=pltpu.CompilerParams(
            collective_id=0, has_side_effects=True, vmem_limit_bytes=67043328
        ),
    )(design, coefficients, response, active_set, lambda_path.T, lambda_index.reshape(1, share))
    return margins, stats[0, :share], stats[1, :share], stats[2, :share]


def solution(mesh):
    return jax.shard_map(
        body,
        mesh=mesh,
        in_specs=(
            P("samp", "feat"),
            P(None, "feat"),
            P(None, "samp"),
            P(None, "feat"),
            P("samp", None),
            P("samp"),
        ),
        out_specs=(P("samp", "feat"), P("samp"), P("samp"), P("samp")),
        check_vma=False,
    )
```

```python
import functools

import jax
import jax.numpy as jnp
from jax import lax
from jax.experimental import pallas as pl
from jax.experimental.pallas import tpu as pltpu
from jax.sharding import PartitionSpec as P

NF = 65536
F32 = jnp.float32
BF16 = jnp.bfloat16
CHUNKS = 4
GROUPS = ((0, 16), (16, 8))
BLOCKS = 4
PARTS = (8, 4)


def split(value):
    high = value.astype(BF16)
    return high, (value - high.astype(F32)).astype(BF16)


def dot(a, b):
    return jnp.dot(a, b, preferred_element_type=F32)


def kernel(
    design, coefficients, response, active, lpath, lindex,
    margins, stats,
    raw, d_all, coef, act, resp, m_a, m_b,
    part, got1, summed, got2, resid, a_a, a_b,
    grad, got_core, got_hop, got_end, lams, peers, early,
    coef_sem, act_sem, load_sem, sent, r1, r2, r3, rc, rx, rt,
):
    samp = lax.axis_index("samp")
    feat = lax.axis_index("feat")
    x, core = samp // 2, samp % 2
    z, y = feat // 4, feat % 4
    rows, samples = response.shape
    features = design.shape[1]
    share = rows // 8
    height = samples // CHUNKS
    masked, residuals = (m_a, m_b), (a_a, a_b)

    def to(s, f):
        return dict(device_id=(s, f), device_id_type=pl.DeviceIdType.MESH)

    def await_bytes(ref, sem):
        pltpu.make_async_copy(ref, ref, sem).wait()

    def rows_of(g):
        return pl.ds(*GROUPS[g])

    partner = 2 * x + 1 - core
    left = 2 * ((x + 3) % 4) + core
    right = 2 * ((x + 1) % 4) + core

    step = features // BLOCKS

    def load_block(b):
        area = pl.ds(pl.multiple_of(b * step, step), step)
        return (
            pltpu.make_async_copy(coefficients.at[:, area], coef.at[:, area], coef_sem.at[b]),
            pltpu.make_async_copy(active.at[:, area], act.at[:, area], act_sem.at[b]))

    def load_design(c):
        area = pl.ds(pl.multiple_of(c * height, height), height)
        return pltpu.make_async_copy(design.at[area], raw.at[area], load_sem.at[c])

    wide = features // 2

    def load_half(h):
        area = pl.ds(0, height), pl.ds(h * wide, wide)
        return pltpu.make_async_copy(design.at[area], raw.at[area], load_sem.at[h * (CHUNKS + 1)])

    load_response = pltpu.make_async_copy(response, resp, load_sem.at[CHUNKS])
    for h in (0, 1):
        for b in (2 * h, 2 * h + 1):
            for load in load_block(b):
                load.start()
        load_half(h).start()

    barrier = pltpu.get_barrier_semaphore()
    for k in range(1, 16):
        pl.semaphore_signal(barrier, inc=1, **to(samp, (feat + k) % 16))
    for s in (partner, left, right):
        pl.semaphore_signal(barrier, inc=1, **to(s, feat))

    eye = lax.broadcasted_iota(jnp.int32, (share, share), 0) == lax.broadcasted_iota(jnp.int32, (share, share), 1)
    positions = lax.broadcasted_iota(jnp.int32, lpath.shape, 0)
    index, path = lindex[...], lpath[...]

    def pick(chosen):
        row = jnp.sum(jnp.where(positions == chosen, path, 0.0), axis=0, keepdims=True)
        return jnp.sum(jnp.where(eye, jnp.broadcast_to(row, (share, share)), 0.0), axis=1, keepdims=True)

    lam_new, lam_old = pick(index), pick(index - 1)
    lams[0] = jnp.broadcast_to(lam_new, (share, 128))
    lams[1] = jnp.broadcast_to(2.0 * lam_new - lam_old, (share, 128))

    @jax.named_scope("mask")
    def mask_step(b, carry):
        for load in load_block(b):
            load.wait()
        area = pl.ds(pl.multiple_of(b * step, step), step)
        value = coef[:, area] * act[:, area].astype(F32)
        high = value.astype(BF16).astype(F32)
        low = value - high
        for (first, count), target in zip(GROUPS, masked):
            pieces = [
                v.reshape(8, share, step)[:, first:first + count].reshape(8 * count, step).astype(BF16)
                for v in (high, low)]
            target[area, :] = jnp.concatenate(pieces, axis=0).T
        return carry


    def along(color, k):
        return 4 * z + (y + k) % 4 if color == 0 else 4 * ((z + k) % 4) + y

    def place(color):
        return y if color == 0 else z

    def lanes_of(c):
        return pl.ds(pl.multiple_of(c * height, height), height)

    def send1(g, c, color, k):
        j = color * 4 + (place(color) + k) % 4
        return pltpu.make_async_remote_copy(
            part.at[c, j, rows_of(g)], got1.at[c, color, k - 1, rows_of(g)],
            sent.at[0], r1.at[g, c], **to(samp, along(color, k)))

    def send2(g, c, color, k):
        return pltpu.make_async_remote_copy(
            summed.at[c, color, rows_of(g)], got2.at[c, color, k - 1, rows_of(g)],
            sent.at[1], r2.at[g, c], **to(samp, along(1 - color, k)))

    def send3(g, c, color, k):
        area = resid.at[color * 4 + place(color), rows_of(g), lanes_of(c)]
        return pltpu.make_async_remote_copy(
            area, area, sent.at[2], r3.at[g, c], **to(samp, along(color, k)))

    def phase0(g, c, fitted=None):
        count = GROUPS[g][1]
        if fitted is None:
            fitted = dot(d_all[c].reshape(2 * height, features), masked[g][...])
        fitted = (fitted[:height] + fitted[height:]).T
        part[c, :, rows_of(g), :] = (fitted[:8 * count] + fitted[8 * count:]).reshape(8, count, height)

    def start1(g, c):
        for k in (2, 1, 3):
            for color in (0, 1):
                send1(g, c, color, k).start()

    def phase1(g, c):
        mine = rows_of(g)
        await_bytes(got1.at[c, :, :, mine], r1.at[g, c])
        for color in (0, 1):
            summed[c, color, mine] = (part[c, color * 4 + place(color), mine] + got1[c, color, 0, mine]) + (
                got1[c, color, 1, mine] + got1[c, color, 2, mine])
            for k in (2, 1, 3):
                send2(g, c, color, k).start()

    def phase2(g, c):
        first, count = GROUPS[g]
        mine = rows_of(g)
        await_bytes(got2.at[c, :, :, mine], r2.at[g, c])
        for color in (0, 1):
            j = color * 4 + place(color)
            total = (summed[c, color, mine] + got2[c, color, 0, mine]) + (got2[c, color, 1, mine] + got2[c, color, 2, mine])
            observed = resp[pl.ds(pl.multiple_of(j * share + first, 8), count), lanes_of(c)]
            resid[j, mine, lanes_of(c)] = observed - total
            for k in (2, 1, 3):
                send3(g, c, color, k).start()

    def phase3(g, c):
        size = 8 * GROUPS[g][1]
        await_bytes(got2.at[c, :, :, rows_of(g)], r3.at[g, c])
        hi, lo = split(resid[:, rows_of(g), lanes_of(c)].reshape(size, height))
        residuals[g][:size, lanes_of(c)] = hi
        residuals[g][size:, lanes_of(c)] = lo

    @jax.named_scope("fita")
    def fit_a(c, carry):
        load_design(c).wait()
        hi, lo = split(raw[pl.ds(pl.multiple_of(c * height, height), height), :])
        d_all[c, 0] = hi
        d_all[c, 1] = lo
        phase0(0, c)
        start1(0, c)
        return carry

    def fit_half(h):
        lax.fori_loop(2 * h, 2 * h + 2, mask_step, 0)
        with jax.named_scope("half"):
            load_half(h).wait()
            load_design(h + 1).start()
            cols = pl.ds(h * wide, wide)
            hi, lo = split(raw[:height, cols])
            d_all[0, 0, :, cols] = hi
            d_all[0, 1, :, cols] = lo
            return dot(d_all[0, :, :, cols].reshape(2 * height, wide), m_a[cols, :])

    @jax.named_scope("fitb")
    def fit_b(c, carry):
        phase1(0, c)
        phase0(1, c)
        start1(1, c)
        return carry

    early[...] = fit_half(0)
    phase0(0, 0, early[...] + fit_half(1))
    for c in range(3, CHUNKS):
        load_design(c).start()
    load_response.start()
    pl.semaphore_wait(barrier, 18)
    start1(0, 0)
    lax.fori_loop(1, CHUNKS, fit_a, 0)
    load_response.wait()
    lax.fori_loop(0, CHUNKS, fit_b, 0)

    x_left, x_right, x_far = (x + 3) % 4, (x + 1) % 4, (x + 2) % 4
    widths = [features // parts for parts in PARTS]

    def cols_of(g, q):
        return pl.ds(pl.multiple_of(q * widths[g], widths[g]), widths[g])

    def halves_of(g, q):
        width, half = widths[g], widths[g] // 2
        return (
            pl.ds(pl.multiple_of(q * width, half), half),
            pl.ds(pl.multiple_of(q * width + half, half), half),
            pl.ds(pl.multiple_of(q * half, half), half))

    def send_core(g, q):
        return pltpu.make_async_remote_copy(
            grad.at[:, 1 - core, rows_of(g), cols_of(g, q)], got_core.at[:, rows_of(g), cols_of(g, q)],
            sent.at[3], rc.at[g * PARTS[0] + q], **to(partner, feat))

    def send_x(g, q, kind):
        near, far, packed = halves_of(g, q)
        mine = rows_of(g)
        source, target, where = (
            (grad.at[x_far, core, mine, near], got_hop.at[0, mine, packed], left),
            (grad.at[x_far, core, mine, far], got_hop.at[1, mine, packed], right),
            (grad.at[x_left, core, mine, far], got_end.at[0, mine, far], left),
            (grad.at[x_right, core, mine, near], got_end.at[1, mine, near], right),
            (grad.at[x_left, core, mine, near], got_end.at[0, mine, near], left),
            (grad.at[x_right, core, mine, far], got_end.at[1, mine, far], right),
        )[kind]
        return pltpu.make_async_remote_copy(source, target, sent.at[4], rx.at[g * PARTS[0] + q, min(kind // 2, 1)], **to(where, feat))

    @jax.named_scope("multiply")
    def multiply(g, q):
        cols, count, width = cols_of(g, q), GROUPS[g][1], widths[g]
        size = 8 * count
        both = dot(residuals[g][...], d_all[:, 0, :, cols].reshape(samples, width))
        value = both[:size] + both[size:] + dot(residuals[g][:size], d_all[:, 1, :, cols].reshape(samples, width))
        for j in range(8):
            grad[j // 2, j % 2, rows_of(g), cols] = value[j * count:(j + 1) * count, :]
        send_core(g, q).start()

    @jax.named_scope("hop1")
    def first_hop(g, q):
        cols, mine = cols_of(g, q), rows_of(g)
        send_core(g, q).wait_recv()
        for j in (x_far, x_left, x_right, x):
            grad[j, core, mine, cols] = grad[j, core, mine, cols] + got_core[j, mine, cols]
        for kind in (0, 1, 2, 3):
            send_x(g, q, kind).start()

    @jax.named_scope("hop2")
    def second_hop(g, q):
        near, far, packed = halves_of(g, q)
        mine = rows_of(g)
        await_bytes(got_hop.at[:, mine, packed], rx.at[g * PARTS[0] + q, 0])
        grad[x_left, core, mine, near] = grad[x_left, core, mine, near] + got_hop[0, mine, packed]
        grad[x_right, core, mine, far] = grad[x_right, core, mine, far] + got_hop[1, mine, packed]
        send_x(g, q, 4).start()
        send_x(g, q, 5).start()

    @jax.named_scope("finish")
    def finish(g, q, carry):
        peak, violation, mass = carry
        first, count = GROUPS[g]
        mine = rows_of(g)
        await_bytes(got_end.at[:, mine, cols_of(g, q)], rx.at[g * PARTS[0] + q, 1])
        own = pl.ds(pl.multiple_of(samp * share + first, 8), count)
        for j in range(0, widths[g], 128):
            cols = pl.ds(pl.multiple_of(q * widths[g] + j, 128), 128)
            magnitude = jnp.abs(grad[x, core, mine, cols] + (got_end[0, mine, cols] + got_end[1, mine, cols]))
            margin = magnitude - lams[1, mine]
            margins[mine, cols] = margin
            peak = jnp.maximum(peak, magnitude)
            violation = violation + (1.0 - act[own, cols].astype(F32)) * jnp.maximum(magnitude - lams[0, mine], 0.0)
            mass = mass + jnp.maximum(margin, 0.0)
        return peak, violation, mass

    def multiply_a(q, carry):
        multiply(0, q)

        @pl.when(q == 1)
        def _():
            first_hop(0, 0)

        @pl.when(q >= 3)
        def _():
            first_hop(0, q - 2)

        @pl.when(q == 2)
        def _():
            phase2(1, CHUNKS - 1)

        return carry

    def multiply_b(q, carry):
        multiply(1, q)

        @pl.when(q >= 1)
        def _():
            first_hop(1, q - 1)

        second_hop(0, q + 3)
        return carry

    with jax.named_scope("phase12"):
        for c in range(CHUNKS):
            phase2(0, c)
            phase1(1, c)
    with jax.named_scope("phase23"):
        for c in range(CHUNKS):
            if c < CHUNKS - 1:
                phase2(1, c)
            phase3(0, c)
    lax.fori_loop(0, PARTS[0], multiply_a, 0)
    first_hop(0, PARTS[0] - 2)
    first_hop(0, PARTS[0] - 1)

    def second_hops(g, first, last):
        lax.fori_loop(first, last, lambda q, carry: (second_hop(g, q), carry)[1], 0)

    second_hops(0, 0, 3)
    with jax.named_scope("phase3"):
        for c in range(CHUNKS):
            phase3(1, c)
    lax.fori_loop(0, PARTS[1], multiply_b, 0)
    first_hop(1, PARTS[1] - 1)
    second_hops(0, 3 + PARTS[1], PARTS[0])
    second_hops(1, 0, PARTS[1])
    carries = [
        lax.fori_loop(0, PARTS[g], functools.partial(finish, g), (jnp.zeros((count, 128), F32),) * 3)
        for g, (_, count) in enumerate(GROUPS)]
    carry = [jnp.concatenate(pair, axis=0) for pair in zip(*carries)]

    with jax.named_scope("stats"):
        peak, violation, mass = carry
        lane = lax.broadcasted_iota(jnp.int32, (share, 128), 1)
        packed = jnp.where(
            lane == 0, jnp.max(peak, axis=1, keepdims=True),
            jnp.where(
                lane == 1, jnp.sum(violation, axis=1, keepdims=True) * (1.0 / NF),
                jnp.where(lane == 2, jnp.sum(mass, axis=1, keepdims=True) * (1.0 / NF), 0.0)))
        packed = jnp.concatenate([packed, jnp.zeros((128 - share, 128), F32)], axis=0).T
        peers[feat] = packed[:8, :]

        def send_stats(k):
            return pltpu.make_async_remote_copy(
                peers.at[feat], peers.at[feat], sent.at[5], rt.at[0], **to(samp, (feat + k) % 16))

        for k in range(1, 16):
            send_stats(k).start()
        await_bytes(peers.at[pl.ds(0, 15)], rt.at[0])
        everything = [peers[k] for k in range(16)]
        largest, total = everything[0], everything[0]
        for k in range(1, 16):
            largest = jnp.maximum(largest, everything[k])
            total = total + everything[k]
        stats[...] = jnp.where(lax.broadcasted_iota(jnp.int32, (8, 128), 0) == 0, largest, total)

    await_bytes(got1, sent.at[0])
    await_bytes(got1, sent.at[1])
    await_bytes(got1, sent.at[2])
    await_bytes(got_core, sent.at[3])
    await_bytes(got_hop, sent.at[4])
    await_bytes(got_end, sent.at[4])
    await_bytes(peers.at[pl.ds(0, 15)], sent.at[5])


def body(design, coefficients, response, active_set, lambda_path, lambda_index):
    samples, features = design.shape
    rows = coefficients.shape[0]
    share = lambda_path.shape[0]
    height = samples // CHUNKS
    vmem = pltpu.VMEM
    dma = pltpu.SemaphoreType.DMA
    everywhere = pl.BlockSpec(memory_space=pl.ANY)
    inside = pl.BlockSpec(memory_space=pltpu.VMEM)
    margins, stats = pl.pallas_call(
        kernel,
        out_shape=(
            vmem((share, features), F32),
            vmem((8, 128), F32),
        ),
        in_specs=[everywhere] * 4 + [inside] * 2,
        out_specs=(inside, inside),
        scratch_shapes=[
            vmem((samples, features), F32),
            vmem((CHUNKS, 2, height, features), BF16),
            vmem((rows, features), F32),
            vmem((rows, features), jnp.int32),
            vmem((rows, samples), F32),
            *[vmem((features, 16 * count), BF16) for _, count in GROUPS],
            vmem((CHUNKS, 8, share, height), F32),
            vmem((CHUNKS, 2, 3, share, height), F32),
            vmem((CHUNKS, 2, share, height), F32),
            vmem((CHUNKS, 2, 3, share, height), F32),
            vmem((8, share, samples), F32),
            *[vmem((16 * count, samples), BF16) for _, count in GROUPS],
            vmem((4, 2, share, features), F32),
            vmem((4, share, features), F32),
            vmem((2, share, features // 2), F32),
            vmem((2, share, features), F32),
            vmem((2, share, 128), F32),
            vmem((16, 8, 128), F32),
            vmem((2 * height, 16 * GROUPS[0][1]), F32),
            dma((BLOCKS,)),
            dma((BLOCKS,)),
            dma((CHUNKS + 2,)),
            dma((6,)),
            *[dma((2, CHUNKS))] * 3,
            dma((sum(PARTS),)),
            dma((sum(PARTS), 2)),
            dma((1,)),
        ],
        compiler_params=pltpu.CompilerParams(
            collective_id=0, has_side_effects=True, vmem_limit_bytes=62 * 1024 * 1024
        ),
    )(design, coefficients, response, active_set, lambda_path.T, lambda_index.reshape(1, share))
    return margins, stats[0, :share], stats[1, :share], stats[2, :share]


def solution(mesh):
    return jax.shard_map(
        body,
        mesh=mesh,
        in_specs=(
            P("samp", "feat"),
            P(None, "feat"),
            P(None, "samp"),
            P(None, "feat"),
            P("samp", None),
            P("samp"),
        ),
        out_specs=(P("samp", "feat"), P("samp"), P("samp"), P("samp")),
        check_vma=False,
    )
```

```python
import functools

import jax
import jax.numpy as jnp
from jax import lax
from jax.experimental import pallas as pl
from jax.experimental.pallas import tpu as pltpu
from jax.sharding import PartitionSpec as P

NF = 65536
F32 = jnp.float32
BF16 = jnp.bfloat16
CHUNKS = 4
GROUPS = ((0, 16), (16, 8))
BLOCKS = 4
PARTS = (8, 4)


def split(value):
    high = value.astype(BF16)
    return high, (value - high.astype(F32)).astype(BF16)


def dot(a, b):
    return jnp.dot(a, b, preferred_element_type=F32)


def kernel(
    design, coefficients, response, active, lpath, lindex,
    margins, stats,
    raw, d_all, coef, act, resp, m_a, m_b,
    part, got1, summed, got2, resid, a_a, a_b,
    grad, got_core, got_hop, got_end, lams, peers, early,
    coef_sem, act_sem, load_sem, sent, r1, r2, r3, rc, rx, rt,
):
    samp = lax.axis_index("samp")
    feat = lax.axis_index("feat")
    x, core = samp // 2, samp % 2
    z, y = feat // 4, feat % 4
    rows, samples = response.shape
    features = design.shape[1]
    share = rows // 8
    height = samples // CHUNKS
    masked, residuals = (m_a, m_b), (a_a, a_b)

    def to(s, f):
        return dict(device_id=(s, f), device_id_type=pl.DeviceIdType.MESH)

    def await_bytes(ref, sem):
        pltpu.make_async_copy(ref, ref, sem).wait()

    def rows_of(g):
        return pl.ds(*GROUPS[g])

    partner = 2 * x + 1 - core
    left = 2 * ((x + 3) % 4) + core
    right = 2 * ((x + 1) % 4) + core

    step = features // BLOCKS

    def load_block(b):
        area = pl.ds(pl.multiple_of(b * step, step), step)
        return (
            pltpu.make_async_copy(coefficients.at[:, area], coef.at[:, area], coef_sem.at[b]),
            pltpu.make_async_copy(active.at[:, area], act.at[:, area], act_sem.at[b]))

    def load_design(c):
        area = pl.ds(pl.multiple_of(c * height, height), height)
        return pltpu.make_async_copy(design.at[area], raw.at[area], load_sem.at[c])

    wide = features // 2

    def load_half(h):
        area = pl.ds(0, height), pl.ds(h * wide, wide)
        return pltpu.make_async_copy(design.at[area], raw.at[area], load_sem.at[h * (CHUNKS + 1)])

    load_response = pltpu.make_async_copy(response, resp, load_sem.at[CHUNKS])
    def load_blocks(first):
        for b in (first, first + 1):
            for load in load_block(b):
                load.start()

    load_blocks(0)
    load_half(0).start()

    barrier = pltpu.get_barrier_semaphore()
    for k in range(1, 16):
        pl.semaphore_signal(barrier, inc=1, **to(samp, (feat + k) % 16))
    for s in (partner, left, right):
        pl.semaphore_signal(barrier, inc=1, **to(s, feat))

    eye = lax.broadcasted_iota(jnp.int32, (share, share), 0) == lax.broadcasted_iota(jnp.int32, (share, share), 1)
    positions = lax.broadcasted_iota(jnp.int32, lpath.shape, 0)
    index, path = lindex[...], lpath[...]

    def pick(chosen):
        row = jnp.sum(jnp.where(positions == chosen, path, 0.0), axis=0, keepdims=True)
        return jnp.sum(jnp.where(eye, jnp.broadcast_to(row, (share, share)), 0.0), axis=1, keepdims=True)

    lam_new, lam_old = pick(index), pick(index - 1)
    lams[0] = jnp.broadcast_to(lam_new, (share, 128))
    lams[1] = jnp.broadcast_to(2.0 * lam_new - lam_old, (share, 128))

    @jax.named_scope("mask")
    def mask_step(b, carry):
        for load in load_block(b):
            load.wait()
        area = pl.ds(pl.multiple_of(b * step, step), step)
        value = coef[:, area] * act[:, area].astype(F32)
        high = value.astype(BF16).astype(F32)
        low = value - high
        for (first, count), target in zip(GROUPS, masked):
            pieces = [
                v.reshape(8, share, step)[:, first:first + count].reshape(8 * count, step).astype(BF16)
                for v in (high, low)]
            target[area, :] = jnp.concatenate(pieces, axis=0).T
        return carry


    def along(color, k):
        return 4 * z + (y + k) % 4 if color == 0 else 4 * ((z + k) % 4) + y

    def place(color):
        return y if color == 0 else z

    def lanes_of(c):
        return pl.ds(pl.multiple_of(c * height, height), height)

    def send1(g, c, color, k):
        j = color * 4 + (place(color) + k) % 4
        return pltpu.make_async_remote_copy(
            part.at[c, j, rows_of(g)], got1.at[c, color, k - 1, rows_of(g)],
            sent.at[0], r1.at[g, c], **to(samp, along(color, k)))

    def send2(g, c, color, k):
        return pltpu.make_async_remote_copy(
            summed.at[c, color, rows_of(g)], got2.at[c, color, k - 1, rows_of(g)],
            sent.at[1], r2.at[g, c], **to(samp, along(1 - color, k)))

    def send3(g, c, color, k):
        area = resid.at[color * 4 + place(color), rows_of(g), lanes_of(c)]
        return pltpu.make_async_remote_copy(
            area, area, sent.at[2], r3.at[g, c], **to(samp, along(color, k)))

    def phase0(g, c, fitted=None):
        count = GROUPS[g][1]
        if fitted is None:
            fitted = dot(d_all[c].reshape(2 * height, features), masked[g][...])
        fitted = (fitted[:height] + fitted[height:]).T
        part[c, :, rows_of(g), :] = (fitted[:8 * count] + fitted[8 * count:]).reshape(8, count, height)

    def start1(g, c):
        for k in (2, 1, 3):
            for color in (0, 1):
                send1(g, c, color, k).start()

    def phase1(g, c):
        mine = rows_of(g)
        await_bytes(got1.at[c, :, :, mine], r1.at[g, c])
        for color in (0, 1):
            summed[c, color, mine] = (part[c, color * 4 + place(color), mine] + got1[c, color, 0, mine]) + (
                got1[c, color, 1, mine] + got1[c, color, 2, mine])
            for k in (2, 1, 3):
                send2(g, c, color, k).start()

    def phase2(g, c):
        first, count = GROUPS[g]
        mine = rows_of(g)
        await_bytes(got2.at[c, :, :, mine], r2.at[g, c])
        for color in (0, 1):
            j = color * 4 + place(color)
            total = (summed[c, color, mine] + got2[c, color, 0, mine]) + (got2[c, color, 1, mine] + got2[c, color, 2, mine])
            observed = resp[pl.ds(pl.multiple_of(j * share + first, 8), count), lanes_of(c)]
            resid[j, mine, lanes_of(c)] = observed - total
            for k in (2, 1, 3):
                send3(g, c, color, k).start()

    def phase3(g, c):
        size = 8 * GROUPS[g][1]
        await_bytes(got2.at[c, :, :, rows_of(g)], r3.at[g, c])
        hi, lo = split(resid[:, rows_of(g), lanes_of(c)].reshape(size, height))
        residuals[g][:size, lanes_of(c)] = hi
        residuals[g][size:, lanes_of(c)] = lo

    @jax.named_scope("fita")
    def fit_a(c, carry):
        load_design(c).wait()
        hi, lo = split(raw[pl.ds(pl.multiple_of(c * height, height), height), :])
        d_all[c, 0] = hi
        d_all[c, 1] = lo
        phase0(0, c)
        start1(0, c)
        return carry

    def fit_half(h):
        with jax.named_scope("half"):
            load_half(h).wait()
            load_design(h + 1).start()
            cols = pl.ds(h * wide, wide)
            hi, lo = split(raw[:height, cols])
            d_all[0, 0, :, cols] = hi
            d_all[0, 1, :, cols] = lo
            return dot(d_all[0, :, :, cols].reshape(2 * height, wide), m_a[cols, :])

    @jax.named_scope("fitb")
    def fit_b(c, carry):
        phase1(0, c)
        phase0(1, c)
        start1(1, c)
        return carry

    lax.fori_loop(0, 1, mask_step, 0)
    load_blocks(2)
    lax.fori_loop(1, 2, mask_step, 0)
    load_half(1).start()
    early[...] = fit_half(0)
    lax.fori_loop(2, BLOCKS, mask_step, 0)
    phase0(0, 0, early[...] + fit_half(1))
    for c in range(3, CHUNKS):
        load_design(c).start()
    load_response.start()
    pl.semaphore_wait(barrier, 18)
    start1(0, 0)
    lax.fori_loop(1, CHUNKS, fit_a, 0)
    load_response.wait()
    lax.fori_loop(0, CHUNKS, fit_b, 0)

    x_left, x_right, x_far = (x + 3) % 4, (x + 1) % 4, (x + 2) % 4
    widths = [features // parts for parts in PARTS]

    def cols_of(g, q):
        return pl.ds(pl.multiple_of(q * widths[g], widths[g]), widths[g])

    def halves_of(g, q):
        width, half = widths[g], widths[g] // 2
        return (
            pl.ds(pl.multiple_of(q * width, half), half),
            pl.ds(pl.multiple_of(q * width + half, half), half),
            pl.ds(pl.multiple_of(q * half, half), half))

    def send_core(g, q):
        return pltpu.make_async_remote_copy(
            grad.at[:, 1 - core, rows_of(g), cols_of(g, q)], got_core.at[:, rows_of(g), cols_of(g, q)],
            sent.at[3], rc.at[g * PARTS[0] + q], **to(partner, feat))

    def send_x(g, q, kind):
        near, far, packed = halves_of(g, q)
        mine = rows_of(g)
        source, target, where = (
            (grad.at[x_far, core, mine, near], got_hop.at[0, mine, packed], left),
            (grad.at[x_far, core, mine, far], got_hop.at[1, mine, packed], right),
            (grad.at[x_left, core, mine, far], got_end.at[0, mine, far], left),
            (grad.at[x_right, core, mine, near], got_end.at[1, mine, near], right),
            (grad.at[x_left, core, mine, near], got_end.at[0, mine, near], left),
            (grad.at[x_right, core, mine, far], got_end.at[1, mine, far], right),
        )[kind]
        return pltpu.make_async_remote_copy(source, target, sent.at[4], rx.at[g * PARTS[0] + q, min(kind // 2, 1)], **to(where, feat))

    @jax.named_scope("multiply")
    def multiply(g, q, first=0, last=CHUNKS):
        cols, count, width = cols_of(g, q), GROUPS[g][1], widths[g]
        size, depth = 8 * count, (last - first) * height
        source = residuals[g][:, first * height:last * height]
        both = dot(source, d_all[first:last, 0, :, cols].reshape(depth, width))
        value = both[:size] + both[size:] + dot(source[:size], d_all[first:last, 1, :, cols].reshape(depth, width))
        for j in range(8):
            piece = value[j * count:(j + 1) * count, :]
            if first > 0:
                piece = piece + grad[j // 2, j % 2, rows_of(g), cols]
            grad[j // 2, j % 2, rows_of(g), cols] = piece
        if last == CHUNKS:
            send_core(g, q).start()

    @jax.named_scope("hop1")
    def first_hop(g, q, kinds=(0, 1, 2, 3)):
        cols, mine = cols_of(g, q), rows_of(g)
        send_core(g, q).wait_recv()
        for j in (x_far, x_left, x_right, x):
            grad[j, core, mine, cols] = grad[j, core, mine, cols] + got_core[j, mine, cols]
        for kind in kinds:
            send_x(g, q, kind).start()

    @jax.named_scope("hop2")
    def second_hop(g, q):
        near, far, packed = halves_of(g, q)
        mine = rows_of(g)
        await_bytes(got_hop.at[:, mine, packed], rx.at[g * PARTS[0] + q, 0])
        grad[x_left, core, mine, near] = grad[x_left, core, mine, near] + got_hop[0, mine, packed]
        grad[x_right, core, mine, far] = grad[x_right, core, mine, far] + got_hop[1, mine, packed]
        send_x(g, q, 4).start()
        send_x(g, q, 5).start()

    @jax.named_scope("finish")
    def finish(g, q, carry):
        peak, violation, mass = carry
        first, count = GROUPS[g]
        mine = rows_of(g)
        await_bytes(got_end.at[:, mine, cols_of(g, q)], rx.at[g * PARTS[0] + q, 1])
        own = pl.ds(pl.multiple_of(samp * share + first, 8), count)
        for j in range(0, widths[g], 128):
            cols = pl.ds(pl.multiple_of(q * widths[g] + j, 128), 128)
            magnitude = jnp.abs(grad[x, core, mine, cols] + (got_end[0, mine, cols] + got_end[1, mine, cols]))
            margin = magnitude - lams[1, mine]
            margins[mine, cols] = margin
            peak = jnp.maximum(peak, magnitude)
            violation = violation + (1.0 - act[own, cols].astype(F32)) * jnp.maximum(magnitude - lams[0, mine], 0.0)
            mass = mass + jnp.maximum(margin, 0.0)
        return peak, violation, mass

    def multiply_a(q, carry):
        multiply(0, q)

        @pl.when(q == 1)
        def _():
            first_hop(0, 0)

        @pl.when(q >= 3)
        def _():
            first_hop(0, q - 2)

        @pl.when(q == 2)
        def _():
            phase2(1, CHUNKS - 1)

        return carry

    with jax.named_scope("phase12"):
        for c in range(CHUNKS):
            phase2(0, c)
            phase1(1, c)
    with jax.named_scope("phase23"):
        for c in range(CHUNKS - 1):
            if c < CHUNKS - 2:
                phase2(1, c)
            phase3(0, c)
    multiply(0, 0, 0, CHUNKS - 1)
    with jax.named_scope("last23"):
        phase2(1, CHUNKS - 2)
        phase3(0, CHUNKS - 1)
    multiply(0, 0, CHUNKS - 1, CHUNKS)
    lax.fori_loop(1, PARTS[0], multiply_a, 0)
    second_hop(0, 0)
    second_hop(0, 1)
    with jax.named_scope("phase3"):
        for c in range(CHUNKS):
            phase3(1, c)
    multiply(1, 0)
    first_hop(0, 6)
    second_hop(0, 2)
    multiply(1, 1)
    first_hop(0, 7)
    second_hop(0, 3)
    multiply(1, 2)
    first_hop(1, 0, (0, 1))
    second_hop(0, 4)
    multiply(1, 3)
    first_hop(1, 1, (0, 1))
    second_hop(0, 5)
    first_hop(1, 2, (0, 1))
    first_hop(1, 3, (0, 1))
    for q in range(PARTS[1]):
        send_x(1, q, 2).start()
        send_x(1, q, 3).start()
    second_hop(0, 6)
    second_hop(0, 7)
    for q in range(PARTS[1]):
        second_hop(1, q)
    carries = [
        lax.fori_loop(0, PARTS[g], functools.partial(finish, g), (jnp.zeros((count, 128), F32),) * 3)
        for g, (_, count) in enumerate(GROUPS)]
    carry = [jnp.concatenate(pair, axis=0) for pair in zip(*carries)]

    with jax.named_scope("stats"):
        peak, violation, mass = carry
        column = jnp.concatenate([
            jnp.max(peak, axis=1, keepdims=True), jnp.zeros((8, 1), F32),
            jnp.sum(violation, axis=1, keepdims=True) * (1.0 / NF), jnp.zeros((8, 1), F32),
            jnp.sum(mass, axis=1, keepdims=True) * (1.0 / NF), jnp.zeros((128 - 3 * share - 16, 1), F32)], axis=0)
        peers[feat] = jnp.broadcast_to(column, (128, 128)).T[:1, :]

        def send_stats(k):
            return pltpu.make_async_remote_copy(
                peers.at[feat], peers.at[feat], sent.at[5], rt.at[0], **to(samp, (feat + k) % 16))

        for k in range(1, 16):
            send_stats(k).start()
        await_bytes(peers.at[pl.ds(0, 15)], rt.at[0])
        everything = [peers[k] for k in range(16)]
        largest, total = everything[0], everything[0]
        for k in range(1, 16):
            largest = jnp.maximum(largest, everything[k])
            total = total + everything[k]
        stats[...] = jnp.where(lax.broadcasted_iota(jnp.int32, (1, 128), 1) < share, largest, total)

    await_bytes(got1, sent.at[0])
    await_bytes(got1, sent.at[1])
    await_bytes(got1, sent.at[2])
    await_bytes(got_core, sent.at[3])
    await_bytes(got_hop, sent.at[4])
    await_bytes(got_end, sent.at[4])
    await_bytes(peers.at[pl.ds(0, 15)], sent.at[5])


def body(design, coefficients, response, active_set, lambda_path, lambda_index):
    samples, features = design.shape
    rows = coefficients.shape[0]
    share = lambda_path.shape[0]
    height = samples // CHUNKS
    vmem = pltpu.VMEM
    dma = pltpu.SemaphoreType.DMA
    everywhere = pl.BlockSpec(memory_space=pl.ANY)
    inside = pl.BlockSpec(memory_space=pltpu.VMEM)
    margins, stats = pl.pallas_call(
        kernel,
        out_shape=(
            vmem((share, features), F32),
            vmem((1, 128), F32),
        ),
        in_specs=[everywhere] * 4 + [inside] * 2,
        out_specs=(inside, inside),
        scratch_shapes=[
            vmem((samples, features), F32),
            vmem((CHUNKS, 2, height, features), BF16),
            vmem((rows, features), F32),
            vmem((rows, features), jnp.int32),
            vmem((rows, samples), F32),
            *[vmem((features, 16 * count), BF16) for _, count in GROUPS],
            vmem((CHUNKS, 8, share, height), F32),
            vmem((CHUNKS, 2, 3, share, height), F32),
            vmem((CHUNKS, 2, share, height), F32),
            vmem((CHUNKS, 2, 3, share, height), F32),
            vmem((8, share, samples), F32),
            *[vmem((16 * count, samples), BF16) for _, count in GROUPS],
            vmem((4, 2, share, features), F32),
            vmem((4, share, features), F32),
            vmem((2, share, features // 2), F32),
            vmem((2, share, features), F32),
            vmem((2, share, 128), F32),
            vmem((16, 1, 128), F32),
            vmem((2 * height, 16 * GROUPS[0][1]), F32),
            dma((BLOCKS,)),
            dma((BLOCKS,)),
            dma((CHUNKS + 2,)),
            dma((6,)),
            *[dma((2, CHUNKS))] * 3,
            dma((sum(PARTS),)),
            dma((sum(PARTS), 2)),
            dma((1,)),
        ],
        compiler_params=pltpu.CompilerParams(
            collective_id=0, has_side_effects=True, vmem_limit_bytes=62 * 1024 * 1024
        ),
    )(design, coefficients, response, active_set, lambda_path.T, lambda_index.reshape(1, share))
    return margins, *(stats[0, k * (share + 8):k * (share + 8) + share] for k in range(3))


def solution(mesh):
    return jax.shard_map(
        body,
        mesh=mesh,
        in_specs=(
            P("samp", "feat"),
            P(None, "feat"),
            P(None, "samp"),
            P(None, "feat"),
            P("samp", None),
            P("samp"),
        ),
        out_specs=(P("samp", "feat"), P("samp"), P("samp"), P("samp")),
        check_vma=False,
    )
```

```python
import functools

import jax
import jax.numpy as jnp
from jax import lax
from jax.experimental import pallas as pl
from jax.experimental.pallas import tpu as pltpu
from jax.sharding import PartitionSpec as P

NF = 65536
F32 = jnp.float32
BF16 = jnp.bfloat16
CHUNKS = 4
GROUPS = ((0, 16), (16, 8))
BLOCKS = 4
PARTS = (8, 4)


def split(value):
    high = value.astype(BF16)
    return high, (value - high.astype(F32)).astype(BF16)


def dot(a, b):
    return jnp.dot(a, b, preferred_element_type=F32)


def kernel(
    design, coefficients, response, active, lpath, lindex,
    margins, stats,
    raw, d_all, coef, act, resp, m_a, m_b,
    part, got1, summed, got2, resid, a_a, a_b,
    grad, got_core, got_hop, got_end, lams, peers, early, path_v, index_v,
    coef_sem, act_sem, load_sem, sent, r1, r2, r3, rc, rx, rt,
):
    samp = lax.axis_index("samp")
    feat = lax.axis_index("feat")
    x, core = samp // 2, samp % 2
    z, y = feat // 4, feat % 4
    rows, samples = response.shape
    features = design.shape[1]
    share = rows // 8
    height = samples // CHUNKS
    masked, residuals = (m_a, m_b), (a_a, a_b)

    def to(s, f):
        return dict(device_id=(s, f), device_id_type=pl.DeviceIdType.MESH)

    def await_bytes(ref, sem):
        pltpu.make_async_copy(ref, ref, sem).wait()

    def rows_of(g):
        return pl.ds(*GROUPS[g])

    partner = 2 * x + 1 - core
    left = 2 * ((x + 3) % 4) + core
    right = 2 * ((x + 1) % 4) + core

    step = features // BLOCKS

    def load_block(b):
        area = pl.ds(pl.multiple_of(b * step, step), step)
        return (
            pltpu.make_async_copy(coefficients.at[:, area], coef.at[:, area], coef_sem.at[b]),
            pltpu.make_async_copy(active.at[:, area], act.at[:, area], act_sem.at[b]))

    def load_design(c):
        area = pl.ds(pl.multiple_of(c * height, height), height)
        return pltpu.make_async_copy(design.at[area], raw.at[area], load_sem.at[c])

    wide = features // 2

    def load_half(h):
        area = pl.ds(0, height), pl.ds(h * wide, wide)
        return pltpu.make_async_copy(design.at[area], raw.at[area], load_sem.at[h * (CHUNKS + 1)])

    load_response = pltpu.make_async_copy(response, resp, load_sem.at[CHUNKS])
    def load_blocks(first):
        for b in (first, first + 1):
            for load in load_block(b):
                load.start()

    load_small = (
        pltpu.make_async_copy(lpath, path_v, load_sem.at[CHUNKS + 2]),
        pltpu.make_async_copy(lindex, index_v, load_sem.at[CHUNKS + 3]))
    load_blocks(0)
    load_half(0).start()

    barrier = pltpu.get_barrier_semaphore()
    for k in range(1, 16):
        pl.semaphore_signal(barrier, inc=1, **to(samp, (feat + k) % 16))
    for s in (partner, left, right):
        pl.semaphore_signal(barrier, inc=1, **to(s, feat))

    @jax.named_scope("mask")
    def mask_step(b, carry):
        for load in load_block(b):
            load.wait()
        area = pl.ds(pl.multiple_of(b * step, step), step)
        value = coef[:, area] * act[:, area].astype(F32)
        high = value.astype(BF16).astype(F32)
        low = value - high
        for (first, count), target in zip(GROUPS, masked):
            pieces = [
                v.reshape(8, share, step)[:, first:first + count].reshape(8 * count, step).astype(BF16)
                for v in (high, low)]
            target[area, :] = jnp.concatenate(pieces, axis=0).T
        return carry


    def along(color, k):
        return 4 * z + (y + k) % 4 if color == 0 else 4 * ((z + k) % 4) + y

    def place(color):
        return y if color == 0 else z

    def lanes_of(c):
        return pl.ds(pl.multiple_of(c * height, height), height)

    def send1(g, c, color, k):
        j = color * 4 + (place(color) + k) % 4
        return pltpu.make_async_remote_copy(
            part.at[c, j, rows_of(g)], got1.at[c, color, k - 1, rows_of(g)],
            sent.at[0], r1.at[g, c], **to(samp, along(color, k)))

    def send2(g, c, color, k):
        return pltpu.make_async_remote_copy(
            summed.at[c, color, rows_of(g)], got2.at[c, color, k - 1, rows_of(g)],
            sent.at[1], r2.at[g, c], **to(samp, along(1 - color, k)))

    def send3(g, c, color, k):
        area = resid.at[color * 4 + place(color), rows_of(g), lanes_of(c)]
        return pltpu.make_async_remote_copy(
            area, area, sent.at[2], r3.at[g, c], **to(samp, along(color, k)))

    def phase0(g, c, fitted=None):
        count = GROUPS[g][1]
        if fitted is None:
            fitted = dot(d_all[c].reshape(2 * height, features), masked[g][...])
        fitted = (fitted[:height] + fitted[height:]).T
        part[c, :, rows_of(g), :] = (fitted[:8 * count] + fitted[8 * count:]).reshape(8, count, height)

    def start1(g, c):
        for k in (2, 1, 3):
            for color in (0, 1):
                send1(g, c, color, k).start()

    def phase1(g, c):
        mine = rows_of(g)
        await_bytes(got1.at[c, :, :, mine], r1.at[g, c])
        for color in (0, 1):
            summed[c, color, mine] = (part[c, color * 4 + place(color), mine] + got1[c, color, 0, mine]) + (
                got1[c, color, 1, mine] + got1[c, color, 2, mine])
            for k in (2, 1, 3):
                send2(g, c, color, k).start()

    def phase2(g, c):
        first, count = GROUPS[g]
        mine = rows_of(g)
        await_bytes(got2.at[c, :, :, mine], r2.at[g, c])
        for color in (0, 1):
            j = color * 4 + place(color)
            total = (summed[c, color, mine] + got2[c, color, 0, mine]) + (got2[c, color, 1, mine] + got2[c, color, 2, mine])
            observed = resp[pl.ds(pl.multiple_of(j * share + first, 8), count), lanes_of(c)]
            resid[j, mine, lanes_of(c)] = observed - total
            for k in (2, 1, 3):
                send3(g, c, color, k).start()

    def phase3(g, c):
        size = 8 * GROUPS[g][1]
        await_bytes(got2.at[c, :, :, rows_of(g)], r3.at[g, c])
        hi, lo = split(resid[:, rows_of(g), lanes_of(c)].reshape(size, height))
        residuals[g][:size, lanes_of(c)] = hi
        residuals[g][size:, lanes_of(c)] = lo

    @jax.named_scope("fita")
    def fit_a(c, carry):
        load_design(c).wait()
        hi, lo = split(raw[pl.ds(pl.multiple_of(c * height, height), height), :])
        d_all[c, 0] = hi
        d_all[c, 1] = lo
        phase0(0, c)
        start1(0, c)
        return carry

    def fit_half(h):
        with jax.named_scope("half"):
            load_half(h).wait()
            load_design(h + 1).start()
            cols = pl.ds(h * wide, wide)
            hi, lo = split(raw[:height, cols])
            d_all[0, 0, :, cols] = hi
            d_all[0, 1, :, cols] = lo
            return dot(d_all[0, :, :, cols].reshape(2 * height, wide), m_a[cols, :])

    @jax.named_scope("fitb")
    def fit_b(c, carry):
        phase1(0, c)
        phase0(1, c)
        start1(1, c)
        return carry

    lax.fori_loop(0, 1, mask_step, 0)
    load_blocks(2)
    lax.fori_loop(1, 2, mask_step, 0)
    load_half(1).start()
    early[...] = fit_half(0)
    lax.fori_loop(2, BLOCKS, mask_step, 0)
    phase0(0, 0, early[...] + fit_half(1))
    for c in range(3, CHUNKS):
        load_design(c).start()
    load_response.start()
    for load in load_small:
        load.start()
    pl.semaphore_wait(barrier, 18)
    start1(0, 0)
    lax.fori_loop(1, CHUNKS, fit_a, 0)
    load_response.wait()
    lax.fori_loop(0, CHUNKS, fit_b, 0)

    x_left, x_right, x_far = (x + 3) % 4, (x + 1) % 4, (x + 2) % 4
    widths = [features // parts for parts in PARTS]

    def cols_of(g, q):
        return pl.ds(pl.multiple_of(q * widths[g], widths[g]), widths[g])

    def halves_of(g, q):
        width, half = widths[g], widths[g] // 2
        return (
            pl.ds(pl.multiple_of(q * width, half), half),
            pl.ds(pl.multiple_of(q * width + half, half), half),
            pl.ds(pl.multiple_of(q * half, half), half))

    def send_core(g, q):
        return pltpu.make_async_remote_copy(
            grad.at[:, 1 - core, rows_of(g), cols_of(g, q)], got_core.at[:, rows_of(g), cols_of(g, q)],
            sent.at[3], rc.at[g * PARTS[0] + q], **to(partner, feat))

    def send_x(g, q, kind):
        near, far, packed = halves_of(g, q)
        mine = rows_of(g)
        source, target, where = (
            (grad.at[x_far, core, mine, near], got_hop.at[0, mine, packed], left),
            (grad.at[x_far, core, mine, far], got_hop.at[1, mine, packed], right),
            (grad.at[x_left, core, mine, far], got_end.at[0, mine, far], left),
            (grad.at[x_right, core, mine, near], got_end.at[1, mine, near], right),
            (grad.at[x_left, core, mine, near], got_end.at[0, mine, near], left),
            (grad.at[x_right, core, mine, far], got_end.at[1, mine, far], right),
        )[kind]
        return pltpu.make_async_remote_copy(source, target, sent.at[4], rx.at[g * PARTS[0] + q, min(kind // 2, 1)], **to(where, feat))

    @jax.named_scope("multiply")
    def multiply(g, q, first=0, last=CHUNKS):
        cols, count, width = cols_of(g, q), GROUPS[g][1], widths[g]
        size, depth = 8 * count, (last - first) * height
        source = residuals[g][:, first * height:last * height]
        both = dot(source, d_all[first:last, 0, :, cols].reshape(depth, width))
        value = both[:size] + both[size:] + dot(source[:size], d_all[first:last, 1, :, cols].reshape(depth, width))
        for j in range(8):
            piece = value[j * count:(j + 1) * count, :]
            if first > 0:
                piece = piece + grad[j // 2, j % 2, rows_of(g), cols]
            grad[j // 2, j % 2, rows_of(g), cols] = piece
        if last == CHUNKS:
            send_core(g, q).start()

    @jax.named_scope("hop1")
    def first_hop(g, q, kinds=(0, 1, 2, 3)):
        cols, mine = cols_of(g, q), rows_of(g)
        send_core(g, q).wait_recv()
        for j in (x_far, x_left, x_right, x):
            grad[j, core, mine, cols] = grad[j, core, mine, cols] + got_core[j, mine, cols]
        for kind in kinds:
            send_x(g, q, kind).start()

    @jax.named_scope("hop2")
    def second_hop(g, q):
        near, far, packed = halves_of(g, q)
        mine = rows_of(g)
        await_bytes(got_hop.at[:, mine, packed], rx.at[g * PARTS[0] + q, 0])
        grad[x_left, core, mine, near] = grad[x_left, core, mine, near] + got_hop[0, mine, packed]
        grad[x_right, core, mine, far] = grad[x_right, core, mine, far] + got_hop[1, mine, packed]
        send_x(g, q, 4).start()
        send_x(g, q, 5).start()

    @jax.named_scope("finish")
    def finish(g, q, carry):
        peak, violation, mass = carry
        first, count = GROUPS[g]
        mine = rows_of(g)
        await_bytes(got_end.at[:, mine, cols_of(g, q)], rx.at[g * PARTS[0] + q, 1])
        own = pl.ds(pl.multiple_of(samp * share + first, 8), count)
        for j in range(0, widths[g], 128):
            cols = pl.ds(pl.multiple_of(q * widths[g] + j, 128), 128)
            magnitude = jnp.abs(grad[x, core, mine, cols] + (got_end[0, mine, cols] + got_end[1, mine, cols]))
            margin = magnitude - lams[1, mine]
            margins[mine, cols] = margin
            peak = jnp.maximum(peak, magnitude)
            violation = violation + (1.0 - act[own, cols].astype(F32)) * jnp.maximum(magnitude - lams[0, mine], 0.0)
            mass = mass + jnp.maximum(margin, 0.0)
        return peak, violation, mass

    def multiply_a(q, carry):
        multiply(0, q)

        @pl.when(q == 1)
        def _():
            first_hop(0, 0)

        @pl.when(q >= 3)
        def _():
            first_hop(0, q - 2)

        @pl.when(q == 2)
        def _():
            phase2(1, CHUNKS - 1)

        return carry

    for load in load_small:
        load.wait()
    eye = lax.broadcasted_iota(jnp.int32, (share, share), 0) == lax.broadcasted_iota(jnp.int32, (share, share), 1)
    positions = lax.broadcasted_iota(jnp.int32, path_v.shape, 0)
    index, path = index_v[...], path_v[...]

    def pick(chosen):
        row = jnp.sum(jnp.where(positions == chosen, path, 0.0), axis=0, keepdims=True)
        return jnp.sum(jnp.where(eye, jnp.broadcast_to(row, (share, share)), 0.0), axis=1, keepdims=True)

    lam_new, lam_old = pick(index), pick(index - 1)
    lams[0] = jnp.broadcast_to(lam_new, (share, 128))
    lams[1] = jnp.broadcast_to(2.0 * lam_new - lam_old, (share, 128))

    with jax.named_scope("phase12"):
        for c in range(CHUNKS):
            phase2(0, c)
            phase1(1, c)
    with jax.named_scope("phase23"):
        for c in range(CHUNKS - 1):
            if c < CHUNKS - 2:
                phase2(1, c)
            phase3(0, c)
    multiply(0, 0, 0, CHUNKS - 1)
    with jax.named_scope("last23"):
        phase2(1, CHUNKS - 2)
        phase3(0, CHUNKS - 1)
    multiply(0, 0, CHUNKS - 1, CHUNKS)
    lax.fori_loop(1, PARTS[0], multiply_a, 0)
    second_hop(0, 0)
    second_hop(0, 1)
    with jax.named_scope("phase3"):
        for c in range(CHUNKS):
            phase3(1, c)
    multiply(1, 0)
    first_hop(0, 6)
    second_hop(0, 2)
    multiply(1, 1)
    first_hop(0, 7)
    second_hop(0, 3)
    multiply(1, 2)
    first_hop(1, 0, (0, 1))
    second_hop(0, 4)
    multiply(1, 3)
    first_hop(1, 1, (0, 1))
    second_hop(0, 5)
    first_hop(1, 2, (0, 1))
    first_hop(1, 3, (0, 1))
    for q in range(PARTS[1]):
        send_x(1, q, 2).start()
        send_x(1, q, 3).start()
    second_hop(0, 6)
    second_hop(0, 7)
    for q in range(PARTS[1]):
        second_hop(1, q)
    carries = [
        lax.fori_loop(0, PARTS[g], functools.partial(finish, g), (jnp.zeros((count, 128), F32),) * 3)
        for g, (_, count) in enumerate(GROUPS)]
    carry = [jnp.concatenate(pair, axis=0) for pair in zip(*carries)]

    with jax.named_scope("stats"):
        peak, violation, mass = carry
        column = jnp.concatenate([
            jnp.max(peak, axis=1, keepdims=True), jnp.zeros((8, 1), F32),
            jnp.sum(violation, axis=1, keepdims=True) * (1.0 / NF), jnp.zeros((8, 1), F32),
            jnp.sum(mass, axis=1, keepdims=True) * (1.0 / NF), jnp.zeros((128 - 3 * share - 16, 1), F32)], axis=0)
        peers[feat] = jnp.broadcast_to(column, (128, 128)).T[:1, :]

        def send_stats(k):
            return pltpu.make_async_remote_copy(
                peers.at[feat], peers.at[feat], sent.at[5], rt.at[0], **to(samp, (feat + k) % 16))

        for k in range(1, 16):
            send_stats(k).start()
        await_bytes(peers.at[pl.ds(0, 15)], rt.at[0])
        everything = [peers[k] for k in range(16)]
        largest, total = everything[0], everything[0]
        for k in range(1, 16):
            largest = jnp.maximum(largest, everything[k])
            total = total + everything[k]
        stats[...] = jnp.where(lax.broadcasted_iota(jnp.int32, (1, 128), 1) < share, largest, total)

    await_bytes(got1, sent.at[0])
    await_bytes(got1, sent.at[1])
    await_bytes(got1, sent.at[2])
    await_bytes(got_core, sent.at[3])
    await_bytes(got_hop, sent.at[4])
    await_bytes(got_end, sent.at[4])
    await_bytes(peers.at[pl.ds(0, 15)], sent.at[5])


def body(design, coefficients, response, active_set, lambda_path, lambda_index):
    samples, features = design.shape
    rows = coefficients.shape[0]
    share = lambda_path.shape[0]
    height = samples // CHUNKS
    vmem = pltpu.VMEM
    dma = pltpu.SemaphoreType.DMA
    everywhere = pl.BlockSpec(memory_space=pl.ANY)
    inside = pl.BlockSpec(memory_space=pltpu.VMEM)
    margins, stats = pl.pallas_call(
        kernel,
        out_shape=(
            vmem((share, features), F32),
            vmem((1, 128), F32),
        ),
        in_specs=[everywhere] * 4 + [pl.BlockSpec(memory_space=pltpu.HBM)] * 2,
        out_specs=(inside, inside),
        scratch_shapes=[
            vmem((samples, features), F32),
            vmem((CHUNKS, 2, height, features), BF16),
            vmem((rows, features), F32),
            vmem((rows, features), jnp.int32),
            vmem((rows, samples), F32),
            *[vmem((features, 16 * count), BF16) for _, count in GROUPS],
            vmem((CHUNKS, 8, share, height), F32),
            vmem((CHUNKS, 2, 3, share, height), F32),
            vmem((CHUNKS, 2, share, height), F32),
            vmem((CHUNKS, 2, 3, share, height), F32),
            vmem((8, share, samples), F32),
            *[vmem((16 * count, samples), BF16) for _, count in GROUPS],
            vmem((4, 2, share, features), F32),
            vmem((4, share, features), F32),
            vmem((2, share, features // 2), F32),
            vmem((2, share, features), F32),
            vmem((2, share, 128), F32),
            vmem((16, 1, 128), F32),
            vmem((2 * height, 16 * GROUPS[0][1]), F32),
            vmem((lambda_path.shape[1], share), F32),
            vmem((1, share), jnp.int32),
            dma((BLOCKS,)),
            dma((BLOCKS,)),
            dma((CHUNKS + 4,)),
            dma((6,)),
            *[dma((2, CHUNKS))] * 3,
            dma((sum(PARTS),)),
            dma((sum(PARTS), 2)),
            dma((1,)),
        ],
        compiler_params=pltpu.CompilerParams(
            collective_id=0, has_side_effects=True, vmem_limit_bytes=62 * 1024 * 1024
        ),
    )(design, coefficients, response, active_set, lambda_path.T, lambda_index.reshape(1, share))
    return margins, *(stats[0, k * (share + 8):k * (share + 8) + share] for k in range(3))


def solution(mesh):
    return jax.shard_map(
        body,
        mesh=mesh,
        in_specs=(
            P("samp", "feat"),
            P(None, "feat"),
            P(None, "samp"),
            P(None, "feat"),
            P("samp", None),
            P("samp"),
        ),
        out_specs=(P("samp", "feat"), P("samp"), P("samp"), P("samp")),
        check_vma=False,
    )
```
